32 devices in a mesh: member: 2 (over x), lat: 16 (over z, y, core).
Axes of the slice: x: 2, y: 2, z: 4, core: 2. Of those that a mesh axis runs over, the one named last changes fastest.
Arguments:
- field: bfloat16 [192, 1440, 256], P(('member', 'lat')), parts along dimension 0, may hold values from -3000 to 3000
- gain: float32 [256], replicated, may hold values from 0.1 to 1.9
- slot_wave: int32 [96], replicated, may hold values from 0 to 96, as said below
- legendre: bfloat16 [96, 96, 96], P('lat'), may hold values from -0.625 to 0.625
- mixing: bfloat16 [96, 2, 256, 256], P('lat'), may hold values from -0.25 to 0.25
Outputs:
- result: bfloat16 [192, 1440, 256], P(('member', 'lat')), parts along dimension 0
The draws below stay inside these ranges and needn't reach their ends.
There are 2 independent parts, one for each index of `member`. The reference program is written for one: setup_inputs(seed, part) draws one part's arguments, and reference() takes and returns one part's arrays. A program takes and returns all parts, laid end to end along the dimension named above; an argument that names none is the same for every part. Nothing has to cross between parts.
Inputs may be any that keep to these rules, and one draw needn't show every extreme that they name: `slot_wave`: each wavenumber 0 to 95 stands in exactly one slot and every other slot holds 96; slots 2k and 2k+1 of one lat index hold wavenumbers adding up to (4k+2)16 - 1 where both are below 96.
All inputs are finite; a program needn't handle non-finite values.
Results may differ from the reference program's by a relative error of at most 0.0085.
Values may be sent and summed in bfloat16 or wider, within the bound.
A program may use at most 64 MiB of HBM per device.

```python
import math
import jax
import jax.numpy as jnp
from jax import lax

C = 256
NLON = 1440
NLAT = 96
DEG = 96
SLOT_DEV = 6
SLOTS = 96
N_LAT = 16


def draw_field(key, part):
    keys = jax.random.split(key, 3)
    rows = jnp.arange(NLAT, dtype=jnp.float32) / NLAT
    wobble = 0.3 * jax.random.normal(keys[0], (NLAT,), jnp.float32)
    chan = 10.0 ** jax.random.uniform(keys[1], (C,), jnp.float32, 0.0, 1.0)
    base = jnp.clip(jax.random.normal(keys[2], (NLAT, NLON, C), jnp.float32), -6.0, 6.0)
    row_exp = rows + wobble
    row_exp = jnp.clip(row_exp, -0.5, 1.5)
    values = base * (10.0 ** row_exp)[:, None, None] * chan[None, None, :]
    return values.astype(jnp.bfloat16)


def draw_slot_wave(key, part):
    rounds = SLOT_DEV
    pairs = (rounds + 1) // 2
    keys = jax.random.split(jax.random.fold_in(key, 17), pairs)
    perms = jax.vmap(lambda k: jax.random.permutation(k, N_LAT))(keys)
    round_ids = jnp.arange(rounds, dtype=jnp.int32)[:, None]
    places = jnp.arange(N_LAT, dtype=jnp.int32)[None, :]
    chosen = perms[round_ids[:, 0] // 2]
    picks = jnp.where(round_ids % 2 == 0, places, N_LAT - 1 - places)
    owner = jnp.take_along_axis(chosen, jnp.broadcast_to(picks, (rounds, N_LAT)), axis=1)
    wave = round_ids * N_LAT + places
    wave = jnp.where(wave < DEG, wave, DEG)
    slot = owner * SLOT_DEV + round_ids
    table = jnp.zeros((SLOTS,), jnp.int32)
    return table.at[slot.reshape(-1)].set(jnp.broadcast_to(wave, (rounds, N_LAT)).reshape(-1).astype(jnp.int32))


def levels(rng, dims, cuts, smallest, high):
    level, own = 1.0, jax.random.fold_in(rng, 6)
    for dim, shards_of in cuts:
        heights = jnp.exp(jax.random.uniform(jax.random.fold_in(own, dim), (shards_of,), jnp.float32, smallest / len(cuts), high / len(cuts)))
        level = level * jnp.repeat(heights, dims[dim] // shards_of).reshape([-1 if axis == dim else 1 for axis in range(len(dims))])
    return level


def noise(key, shape, scale, reach, cuts=(), kind=jnp.bfloat16):
    result = jax.random.normal(key, shape, jnp.float32) * scale
    if len(cuts) > 0:
        result = levels(key, shape, cuts, -0.22, 0.18) * result
    return jnp.clip(result, min=-reach, max=reach).astype(kind)


def setup_inputs(seed: int = 0, part: int = 0) -> dict:
    key_of = jax.random.split(jax.random.key(seed), 6)
    part_keys = jax.random.split(jax.random.fold_in(key_of[5], part), 6)
    field = draw_field(jax.random.fold_in(jax.random.fold_in(key_of[5], part), 71), part)
    gain = jnp.clip(1.0 + 0.18 * jax.random.normal(key_of[1], (C,), jnp.float32), 0.1, 1.9)
    slot_wave = draw_slot_wave(jax.random.fold_in(key_of[5], 71), part)
    legendre = noise(key_of[3], (SLOTS, DEG, NLAT), NLAT ** -0.5, 0.625, ((0, 16),))
    mixing = noise(key_of[4], (SLOTS, 2, C, C), (2 * C) ** -0.5, 0.25, ((0, 16),))
    return {"field": field, "gain": gain, "slot_wave": slot_wave, "legendre": legendre, "mixing": mixing}


def phase_tables(waves, width):
    points = jnp.arange(width, dtype=jnp.int32)
    phase = (waves[:, None] * points[None, :] % width).astype(jnp.float32) * (2.0 * math.pi / width)
    return (jnp.cos(phase), jnp.sin(phase))

def block_weight(mixing):
    real_part = mixing[:, 0]
    imag_part = mixing[:, 1]
    upper = jnp.concatenate([real_part, imag_part], axis=2)
    lower = jnp.concatenate([-imag_part, real_part], axis=2)
    return jnp.concatenate([upper, lower], axis=1)

def reference(field, gain, slot_wave, legendre, mixing):
    values = field.astype(jnp.float32)
    mean = lax.optimization_barrier(jnp.mean(values, axis=(0, 1)))
    var = lax.optimization_barrier(jnp.mean((values - mean) ** 2, axis=(0, 1)))
    normed = ((values - mean) * (gain / jnp.sqrt(var + 1e-05))).astype(jnp.bfloat16)
    cosine, sine = phase_tables(slot_wave, NLON)
    forward = jnp.stack([cosine, -sine]).astype(jnp.bfloat16)
    weight_m = jnp.where(slot_wave == 0, 1.0, 2.0).astype(jnp.float32)[:, None]
    inverse = jnp.stack([weight_m * cosine, -weight_m * sine]).astype(jnp.bfloat16)
    inv_root = 1.0 / math.sqrt(NLON)
    spectrum = jnp.einsum('anc,rkn->karc', normed.astype(jnp.float32), forward.astype(jnp.float32)) * inv_root
    spectrum = spectrum.astype(jnp.bfloat16).reshape(SLOTS, NLAT, 2 * C)
    big = block_weight(mixing)
    lat_scale = math.sqrt(NLAT / DEG)
    degrees = jnp.arange(DEG, dtype=jnp.int32)

    def one_slot(items):
        table, spec, weight, wave = items
        coef = jnp.dot(table, spec, preferred_element_type=jnp.float32)
        coef = jnp.where((degrees >= wave)[:, None], coef, 0.0).astype(jnp.bfloat16)
        mixed = jnp.dot(coef, weight, preferred_element_type=jnp.float32).astype(jnp.bfloat16)
        back = jnp.dot(table.T, mixed, preferred_element_type=jnp.float32) * lat_scale
        return back.astype(jnp.bfloat16)
    back = lax.map(one_slot, (legendre, spectrum, big, slot_wave))
    back = back.reshape(SLOTS, NLAT, 2, C)
    filtered = jnp.einsum('karc,rkn->anc', back.astype(jnp.float32), inverse.astype(jnp.float32)) * inv_root
    return (normed.astype(jnp.float32) + filtered).astype(jnp.bfloat16)
```

```python
import functools
import math

import jax
import jax.numpy as jnp
import numpy as np
from jax import lax
from jax.experimental import pallas as pl
from jax.experimental.pallas import tpu as pltpu
from jax.sharding import PartitionSpec as P

MESH = pl.DeviceIdType.MESH
F32 = jnp.float32
BF16 = jnp.bfloat16


def wave_table(degs, width):
    pad = -(-(degs + 1) // 128) * 128
    waves = np.arange(degs + 1)[:, None]
    phase = (waves * np.arange(width)[None, :] % width) * (2.0 * np.pi / width)
    table = np.zeros((2, pad, width), np.float32)
    table[0, : degs + 1] = np.cos(phase)
    table[1, : degs + 1] = -np.sin(phase)
    return table.reshape(2 * pad, width).astype(BF16), pad


def dot(a, b):
    return jnp.dot(a, b, preferred_element_type=F32)


def partner(me, step, count):
    if count & (count - 1):
        return lax.rem(me + step, count)
    out = 0
    for bit in range(count.bit_length() - 1):
        size = 2**bit
        mine = lax.rem(me // size, 2)
        flip = lax.rem(step // size, 2)
        out = out + size * (mine + flip - 2 * mine * flip)
    return out


def exchange_kernel(
    count,
    pad,
    field_ref, wave_ref, target_ref, gain_ref, table_ref, tsum_ref, tsum_row_ref, legendre_ref, mixing_ref,
    ret_ref, stat_ref,
    field_v, mix_v, select, raw, spec, send, recv, back_send, stat_src, stat_recv, lbig,
    field_sem, mix_sem, stat_sems, fwd_sems, back_sems,
):
    me = lax.axis_index("lat")
    lat_dev, width, chans = field_v.shape
    slot_dev, degs, nlat = legendre_ref.shape
    groups, lat_pairs = slot_dev // 2, lat_dev // 2
    rows = count * 8
    others = count - 1
    inv_root = 1.0 / math.sqrt(width)
    total_cells = float(lat_dev * count * width)

    barrier = pltpu.get_barrier_semaphore()

    def greet(step, carry):
        pl.semaphore_signal(barrier, inc=1, device_id={"lat": partner(me, step, count)}, device_id_type=MESH)
        return carry

    lax.fori_loop(1, count, greet, 0)
    loads = []
    for a in range(lat_dev):
        load = pltpu.make_async_copy(field_ref.at[a], field_v.at[a], field_sem.at[a])
        load.start()
        loads.append(load)
    mix_load = pltpu.make_async_copy(mixing_ref, mix_v, mix_sem)
    mix_load.start()

    columns = lax.broadcasted_iota(jnp.int32, (rows, 4 * pad), 1)
    for k in range(groups):
        select[k] = jnp.where(columns == target_ref[k], 1.0, 0.0).astype(BF16)

    squares = jnp.zeros((8, chans), F32)
    sums = jnp.zeros((1, chans), F32)
    for a in range(lat_dev):
        loads[a].wait()
        raw[a] = dot(table_ref[...], field_v[a])
        sums = sums + raw[a, 0:1, :]
        values = field_v[a].astype(F32)
        squares = squares + jnp.sum((values * values).reshape(width // 8, 8, chans), axis=0)
    square = jnp.sum(squares, axis=0, keepdims=True)
    own = jnp.concatenate([sums, square], axis=0)
    stat_src[...] = own
    stat_recv[pl.ds(me, 1)] = own[None]
    local_mean = sums / float(lat_dev * width)

    pl.semaphore_wait(barrier, others)

    def start_stat(step, carry):
        to = partner(me, count - step, count)
        pltpu.make_async_remote_copy(
            src_ref=stat_src, dst_ref=stat_recv.at[me], send_sem=stat_sems.at[0], recv_sem=stat_sems.at[1],
            device_id={"lat": to}, device_id_type=MESH,
        ).start()
        return carry

    lax.fori_loop(1, count, start_stat, 0)

    def start_group(k, source, target, sems):
        def body(step, carry):
            to = partner(me, count - step, count)
            pltpu.make_async_remote_copy(
                src_ref=source.at[k, to], dst_ref=target.at[k, me], send_sem=sems.at[0, k], recv_sem=sems.at[1, k],
                device_id={"lat": to}, device_id_type=MESH,
            ).start()
            return carry

        lax.fori_loop(1, count, body, 0)

    def wait_bytes(ref, sem):
        pltpu.make_async_copy(ref, ref, sem).wait()

    half = 2 * pad
    for p in range(lat_pairs):
        for parity in range(2):
            spec[p, parity * half : (parity + 1) * half, :] = (
                raw[2 * p + parity] - tsum_ref[...] * local_mean
            ).astype(BF16)
    for k in range(groups):
        for p in range(lat_pairs):
            picked = dot(select[k], spec[p])
            send[k, :, p] = picked.reshape(count, 8, chans).astype(BF16)
        recv[k, pl.ds(me, 1)] = send[k, pl.ds(me, 1)]
        start_group(k, send, recv, fwd_sems)

    col = lax.broadcasted_iota(jnp.int32, (nlat, 4 * nlat), 1)
    lat_row = lax.broadcasted_iota(jnp.int32, (nlat, 4 * nlat), 0)
    degree = lax.broadcasted_iota(jnp.int32, (degs, nlat), 0)
    for k in range(groups):
        for jj in range(2):
            slot = 2 * k + jj
            wave = wave_ref[me * slot_dev + slot]
            kept = jnp.where(degree >= wave, legendre_ref[slot].astype(F32), 0.0).astype(BF16)
            for r in range(2):
                q = 2 * jj + r
                spread = jnp.where(col == 4 * lat_row + q, 1.0, 0.0).astype(BF16)
                lbig[k, q * degs : (q + 1) * degs, :] = dot(kept, spread).astype(BF16)

    wait_bytes(stat_recv.at[pl.ds(0, others)], stat_sems.at[1])
    stats = stat_recv[...]
    total = jnp.sum(stats, axis=0)
    mean = total[0:1] / total_cells
    var = total[1:2] / total_cells - mean * mean
    scale = gain_ref[...] / jnp.sqrt(var + 1e-05)
    stat_ref[0:1] = mean
    stat_ref[1:2] = scale
    shift = (stats[:, 0, :] / float(lat_dev * width) - mean).astype(BF16)
    owner = lax.broadcasted_iota(jnp.int32, (4 * nlat, count), 1)
    lat_of = lax.broadcasted_iota(jnp.int32, (4 * nlat, count), 0)
    owned = jnp.where((lat_of >= owner * (4 * lat_dev)) & (lat_of < (owner + 1) * (4 * lat_dev)), 1.0, 0.0).astype(BF16)
    shift_lat = dot(owned, shift).astype(BF16)
    mode_scale = scale * inv_root
    lanes = lax.broadcasted_iota(jnp.int32, (1, 2 * pad), 1)
    mix_load.wait()

    for k in range(groups):
        wait_bytes(recv.at[k, pl.ds(0, others)], fwd_sems.at[1, k])
        arrived = recv[k].astype(F32).reshape(count * lat_pairs * 8, chans).astype(BF16)
        coef = dot(lbig[k], arrived)
        offset = dot(lbig[k], shift_lat)
        mixed = []
        for jj in range(2):
            slot = 2 * k + jj
            wave = wave_ref[me * slot_dev + slot]
            parts = []
            for r in range(2):
                q = slice((2 * jj + r) * degs, (2 * jj + r + 1) * degs)
                tsum = jnp.sum(jnp.where(lanes == wave + r * pad, tsum_row_ref[...], 0.0), axis=1, keepdims=True)
                parts.append(((coef[q] + tsum * offset[q]) * mode_scale).astype(BF16))
            both = jnp.concatenate(parts, axis=0)
            by_real = dot(both, mix_v[slot, 0])
            by_imag = dot(both, mix_v[slot, 1])
            weight = jnp.where(wave == 0, 1.0, 2.0) * math.sqrt(nlat / degs)
            mixed.append(((by_real[:degs] - by_imag[degs:]) * weight).astype(BF16))
            mixed.append(((by_imag[:degs] + by_real[degs:]) * weight).astype(BF16))
        mixed = jnp.concatenate(mixed, axis=0)
        back = lax.dot_general(lbig[k], mixed, (((0,), (0,)), ((), ())), preferred_element_type=F32)
        back_send[k] = back.reshape(count, lat_pairs, 8, chans).astype(BF16)
        ret_ref[k, pl.ds(me, 1)] = back_send[k, pl.ds(me, 1)]
        start_group(k, back_send, ret_ref, back_sems)

    wait_bytes(stat_recv.at[pl.ds(0, others)], stat_sems.at[0])
    for k in range(groups):
        wait_bytes(send.at[k, pl.ds(0, others)], fwd_sems.at[0, k])
    for k in range(groups):
        wait_bytes(ret_ref.at[k, pl.ds(0, others)], back_sems.at[1, k])
        wait_bytes(back_send.at[k, pl.ds(0, others)], back_sems.at[0, k])


def inverse_kernel(pad, ret_ref, target_ref, stat_ref, table_ref, field_ref, out_ref):
    groups, count, lat_pairs, _, chans = ret_ref.shape
    width = field_ref.shape[1]
    inv_root = 1.0 / math.sqrt(width)
    a = pl.program_id(0)
    pair, parity = a // 2, lax.rem(a, 2)
    rows = count * 8
    line = lax.broadcasted_iota(jnp.int32, (2 * pad, rows), 0) + parity * (2 * pad)
    waves = jnp.zeros((2 * pad, chans), F32)
    for k in range(groups):
        block = ret_ref[k, :, pl.ds(pair, 1)].astype(F32).reshape(rows, chans).astype(BF16)
        waves = waves + dot(jnp.where(line == target_ref[k], 1.0, 0.0).astype(BF16), block)
    filtered = dot(table_ref[...], waves.astype(BF16)) * inv_root
    normed = ((field_ref[0].astype(F32) - stat_ref[0:1]) * stat_ref[1:2]).astype(BF16)
    out_ref[0] = (normed.astype(F32) + filtered).astype(BF16)


def per_device(field, gain, slot_wave, legendre, mixing):
    count = lax.axis_size("lat")
    lat_dev, width, chans = field.shape
    slot_dev, degs, nlat = legendre.shape
    groups, lat_pairs = slot_dev // 2, lat_dev // 2
    table, pad = wave_table(degs, width)
    tsum = table.astype(np.float64).sum(axis=1).astype(np.float32)
    rows = count * 8
    waves = slot_wave.reshape(count, groups, 1, 2, 1).transpose(1, 0, 2, 3, 4)
    offsets = (np.arange(2).reshape(2, 1, 1) * 2 + np.arange(2).reshape(1, 1, 2)) * pad
    target = (waves + jnp.asarray(offsets, jnp.int32)).reshape(groups, rows)

    vmem = pl.BlockSpec(memory_space=pltpu.VMEM)
    anywhere = pl.BlockSpec(memory_space=pl.ANY)
    dma = pltpu.SemaphoreType.DMA
    block = (groups, count, lat_pairs, 8, chans)
    ret, stat = pl.pallas_call(
        functools.partial(exchange_kernel, count, pad),
        out_shape=(jax.ShapeDtypeStruct(block, BF16), jax.ShapeDtypeStruct((2, chans), F32)),
        in_specs=[anywhere, pl.BlockSpec(memory_space=pltpu.SMEM), vmem, vmem, vmem, vmem, vmem, vmem, anywhere],
        out_specs=(vmem, vmem),
        scratch_shapes=[
            pltpu.VMEM(field.shape, BF16),
            pltpu.VMEM(mixing.shape, BF16),
            pltpu.VMEM((groups, rows, 4 * pad), BF16),
            pltpu.VMEM((lat_dev, 2 * pad, chans), F32),
            pltpu.VMEM((lat_pairs, 4 * pad, chans), BF16),
            pltpu.VMEM(block, BF16),
            pltpu.VMEM(block, BF16),
            pltpu.VMEM(block, BF16),
            pltpu.VMEM((2, chans), F32),
            pltpu.VMEM((count, 2, chans), F32),
            pltpu.VMEM((groups, 4 * degs, 4 * nlat), BF16),
            dma((lat_dev,)),
            dma(()),
            dma((2,)),
            dma((2, groups)),
            dma((2, groups)),
        ],
        compiler_params=pltpu.CompilerParams(
            collective_id=0, has_side_effects=True, vmem_limit_bytes=60 * 2**20
        ),
        name="exchange",
    )(
        field, slot_wave, target.reshape(groups, rows, 1), gain.reshape(1, chans), jnp.asarray(table),
        jnp.asarray(tsum.reshape(-1, 1)), jnp.asarray(tsum.reshape(1, -1)), legendre, mixing,
    )
    whole = lambda shape: pl.BlockSpec(shape, lambda a: (0,) * len(shape))
    row_block = pl.BlockSpec((1, width, chans), lambda a: (a, 0, 0))
    return pl.pallas_call(
        functools.partial(inverse_kernel, pad),
        grid=(lat_dev,),
        out_shape=jax.ShapeDtypeStruct(field.shape, BF16),
        in_specs=[whole(block), whole((groups, 1, rows)), whole((2, chans)), whole((width, 2 * pad)), row_block],
        out_specs=row_block,
        compiler_params=pltpu.CompilerParams(vmem_limit_bytes=48 * 2**20),
        name="inverse",
    )(ret, target.reshape(groups, 1, rows), stat, jnp.asarray(table.T.copy()), field)


def solution(mesh):
    return jax.shard_map(
        per_device,
        mesh=mesh,
        in_specs=(
            P(("member", "lat"), None, None),
            P(),
            P(),
            P("lat", None, None),
            P("lat", None, None, None),
        ),
        out_specs=P(("member", "lat"), None, None),
        check_vma=False,
    )
```

```python
import functools
import math

import jax
import jax.numpy as jnp
import numpy as np
from jax import lax
from jax.experimental import pallas as pl
from jax.experimental.pallas import tpu as pltpu
from jax.sharding import PartitionSpec as P

MESH = pl.DeviceIdType.MESH
F32 = jnp.float32
BF16 = jnp.bfloat16


def wave_table(degs, width):
    pad = -(-(degs + 1) // 128) * 128
    waves = np.arange(degs + 1)[:, None]
    phase = (waves * np.arange(width)[None, :] % width) * (2.0 * np.pi / width)
    table = np.zeros((2, pad, width), np.float32)
    table[0, : degs + 1] = np.cos(phase)
    table[1, : degs + 1] = -np.sin(phase)
    return table.reshape(2 * pad, width).astype(BF16), pad


def dot(a, b):
    return jnp.dot(a, b, preferred_element_type=F32)


def partner(me, step, count):
    if count & (count - 1):
        return lax.rem(me + step, count)
    out = 0
    for bit in range(count.bit_length() - 1):
        size = 2**bit
        mine = lax.rem(me // size, 2)
        flip = lax.rem(step // size, 2)
        out = out + size * (mine + flip - 2 * mine * flip)
    return out


def exchange_kernel(
    count,
    pad,
    field_ref, wave_hbm, wave_row_hbm, gain_hbm, table_hbm, tsum_hbm, legendre_hbm, mixing_hbm,
    ret_ref, target_ref, field_v,
    wave_ref, wave_row_ref, gain_ref, table_ref, tsum_row_ref, legendre_ref, mix_v,
    select, raw, spec, send, recv, back_send, stat_src, stat_recv, lbig,
    field_sem, load_sem, stat_sems, fwd_sems, back_sems,
):
    me = lax.axis_index("lat")
    lat_dev, width, chans = field_v.shape
    slot_dev, degs, nlat = legendre_ref.shape
    groups, lat_pairs = slot_dev // 2, lat_dev // 2
    rows = count * 8
    others = count - 1
    inv_root = 1.0 / math.sqrt(width)
    total_cells = float(lat_dev * count * width)

    barrier = pltpu.get_barrier_semaphore()

    def greet(step, carry):
        pl.semaphore_signal(barrier, inc=1, device_id={"lat": partner(me, step, count)}, device_id_type=MESH)
        return carry

    def load_of(index, source, target):
        load = pltpu.make_async_copy(source, target, load_sem.at[index])
        load.start()
        return load

    row_load = load_of(0, wave_row_hbm, wave_row_ref)
    table_load = load_of(1, table_hbm, table_ref)
    tsum_load = load_of(2, tsum_hbm, tsum_row_ref)
    loads = []
    for a in range(lat_dev):
        load = pltpu.make_async_copy(field_ref.at[a], field_v.at[a], field_sem.at[a])
        load.start()
        loads.append(load)
    late = [
        load_of(3, wave_hbm, wave_ref),
        load_of(4, legendre_hbm, legendre_ref),
        load_of(5, gain_hbm, gain_ref),
        load_of(6, mixing_hbm, mix_v),
    ]
    lax.fori_loop(1, count, greet, 0)

    slots = count * slot_dev
    row_load.wait()
    wave_row = wave_row_ref[...].astype(F32)
    columns = lax.broadcasted_iota(jnp.int32, (rows, 4 * pad), 1).astype(F32)
    row = lax.broadcasted_iota(jnp.int32, (rows, 1), 0)
    slot_lane = lax.broadcasted_iota(jnp.int32, (rows, slots), 1)
    for k in range(groups):
        slot_of = row // 8 * slot_dev + 2 * k + row % 4 // 2
        wave_of = jnp.sum(jnp.where(slot_lane == slot_of, wave_row, 0.0), axis=1, keepdims=True)
        target = wave_of + ((row % 8 // 4 * 2 + row % 2) * pad).astype(F32)
        select[k] = jnp.where(columns == target, 1.0, 0.0).astype(BF16)

    tsum_load.wait()
    part_a = lax.broadcasted_iota(jnp.int32, (2 * pad, 2 * pad), 0)
    part_b = lax.broadcasted_iota(jnp.int32, (2 * pad, 2 * pad), 1)
    tsum_col = jnp.sum(jnp.where(part_a == part_b, tsum_row_ref[...], 0.0), axis=1, keepdims=True)
    table_load.wait()
    squares = jnp.zeros((8, chans), F32)
    sums = jnp.zeros((1, chans), F32)
    for a in range(lat_dev):
        loads[a].wait()
        raw[a] = dot(table_ref[...], field_v[a])
        sums = sums + raw[a, 0:1, :]
        values = field_v[a].astype(F32)
        squares = squares + jnp.sum((values * values).reshape(width // 8, 8, chans), axis=0)
    square = jnp.sum(squares, axis=0, keepdims=True)
    own = jnp.concatenate([sums, square], axis=0)
    stat_src[...] = own
    stat_recv[pl.ds(me, 1)] = own[None]
    local_mean = sums / float(lat_dev * width)

    pl.semaphore_wait(barrier, others)

    def start_stat(step, carry):
        to = partner(me, count - step, count)
        pltpu.make_async_remote_copy(
            src_ref=stat_src, dst_ref=stat_recv.at[me], send_sem=stat_sems.at[0], recv_sem=stat_sems.at[1],
            device_id={"lat": to}, device_id_type=MESH,
        ).start()
        return carry

    lax.fori_loop(1, count, start_stat, 0)

    def start_group(k, source, target, sems):
        def body(step, carry):
            to = partner(me, count - step, count)
            pltpu.make_async_remote_copy(
                src_ref=source.at[k, to], dst_ref=target.at[k, me], send_sem=sems.at[0, k], recv_sem=sems.at[1, k],
                device_id={"lat": to}, device_id_type=MESH,
            ).start()
            return carry

        lax.fori_loop(1, count, body, 0)

    def wait_bytes(ref, sem):
        pltpu.make_async_copy(ref, ref, sem).wait()

    half = 2 * pad
    for p in range(lat_pairs):
        for parity in range(2):
            spec[p, parity * half : (parity + 1) * half, :] = (
                raw[2 * p + parity] - tsum_col * local_mean
            ).astype(BF16)
    for k in range(groups):
        for p in range(lat_pairs):
            picked = dot(select[k], spec[p])
            send[k, :, p] = picked.reshape(count, 8, chans).astype(BF16)
        recv[k, pl.ds(me, 1)] = send[k, pl.ds(me, 1)]
        start_group(k, send, recv, fwd_sems)

    for load in late:
        load.wait()
    slot_a = lax.broadcasted_iota(jnp.int32, (slots, slots), 0)
    slot_b = lax.broadcasted_iota(jnp.int32, (slots, slots), 1)
    wave_col = jnp.sum(jnp.where(slot_a == slot_b, wave_row, 0.0), axis=1, keepdims=True)
    lane = lax.broadcasted_iota(jnp.int32, (1, rows), 1)
    slot_line = lax.broadcasted_iota(jnp.int32, (slots, rows), 0)
    for k in range(groups):
        slot_of = lane // 8 * slot_dev + 2 * k + lane % 4 // 2
        wave_of = jnp.sum(jnp.where(slot_line == slot_of, wave_col, 0.0), axis=0, keepdims=True)
        target_ref[:, k * rows : (k + 1) * rows] = wave_of + ((lane % 8 // 4 * 2 + lane % 2) * pad).astype(F32)

    col = lax.broadcasted_iota(jnp.int32, (nlat, 4 * nlat), 1)
    lat_row = lax.broadcasted_iota(jnp.int32, (nlat, 4 * nlat), 0)
    degree = lax.broadcasted_iota(jnp.int32, (degs, nlat), 0)
    for k in range(groups):
        for jj in range(2):
            slot = 2 * k + jj
            wave = wave_ref[me * slot_dev + slot]
            kept = jnp.where(degree >= wave, legendre_ref[slot].astype(F32), 0.0).astype(BF16)
            for r in range(2):
                q = 2 * jj + r
                spread = jnp.where(col == 4 * lat_row + q, 1.0, 0.0).astype(BF16)
                lbig[k, q * degs : (q + 1) * degs, :] = dot(kept, spread).astype(BF16)

    wait_bytes(stat_recv.at[pl.ds(0, others)], stat_sems.at[1])
    stats = stat_recv[...]
    total = jnp.sum(stats, axis=0)
    mean = total[0:1] / total_cells
    var = total[1:2] / total_cells - mean * mean
    scale = gain_ref[...] / jnp.sqrt(var + 1e-05)
    shift = (stats[:, 0, :] / float(lat_dev * width) - mean).astype(BF16)
    owner = lax.broadcasted_iota(jnp.int32, (4 * nlat, count), 1)
    lat_of = lax.broadcasted_iota(jnp.int32, (4 * nlat, count), 0)
    owned = jnp.where((lat_of >= owner * (4 * lat_dev)) & (lat_of < (owner + 1) * (4 * lat_dev)), 1.0, 0.0).astype(BF16)
    shift_lat = dot(owned, shift).astype(BF16)
    mode_scale = scale * inv_root
    lanes = lax.broadcasted_iota(jnp.int32, (1, 2 * pad), 1)

    def normalize(a):
        field_v[a] = ((field_v[a].astype(F32) - mean) * scale).astype(BF16)

    for k in range(groups):
        if k > 0:
            for a in range((k - 1) * lat_dev // groups, k * lat_dev // groups):
                normalize(a)
        wait_bytes(recv.at[k, pl.ds(0, others)], fwd_sems.at[1, k])
        arrived = recv[k].astype(F32).reshape(count * lat_pairs * 8, chans).astype(BF16)
        coef = dot(lbig[k], arrived)
        offset = dot(lbig[k], shift_lat)
        mixed = []
        for jj in range(2):
            slot = 2 * k + jj
            wave = wave_ref[me * slot_dev + slot]
            parts = []
            for r in range(2):
                q = slice((2 * jj + r) * degs, (2 * jj + r + 1) * degs)
                tsum = jnp.sum(jnp.where(lanes == wave + r * pad, tsum_row_ref[...], 0.0), axis=1, keepdims=True)
                parts.append(((coef[q] + tsum * offset[q]) * mode_scale).astype(BF16))
            both = jnp.concatenate(parts, axis=0)
            by_real = dot(both, mix_v[slot, 0])
            by_imag = dot(both, mix_v[slot, 1])
            weight = jnp.where(wave == 0, 1.0, 2.0) * (math.sqrt(nlat / degs) * inv_root)
            mixed.append(((by_real[:degs] - by_imag[degs:]) * weight).astype(BF16))
            mixed.append(((by_imag[:degs] + by_real[degs:]) * weight).astype(BF16))
        mixed = jnp.concatenate(mixed, axis=0)
        back = lax.dot_general(lbig[k], mixed, (((0,), (0,)), ((), ())), preferred_element_type=F32)
        back_send[k] = back.reshape(count, lat_pairs, 8, chans).astype(BF16)
        ret_ref[k, pl.ds(me, 1)] = back_send[k, pl.ds(me, 1)]
        start_group(k, back_send, ret_ref, back_sems)

    for a in range((groups - 1) * lat_dev // groups, lat_dev):
        normalize(a)
    wait_bytes(stat_recv.at[pl.ds(0, others)], stat_sems.at[0])
    for k in range(groups):
        wait_bytes(send.at[k, pl.ds(0, others)], fwd_sems.at[0, k])
    for k in range(groups):
        wait_bytes(ret_ref.at[k, pl.ds(0, others)], back_sems.at[1, k])
        wait_bytes(back_send.at[k, pl.ds(0, others)], back_sems.at[0, k])


def inverse_kernel(pad, ret_ref, target_ref, table_ref, normed_ref, out_ref):
    groups, count, lat_pairs, _, chans = ret_ref.shape
    a = pl.program_id(0)
    pair, parity = a // 2, lax.rem(a, 2)
    rows = groups * count * 8
    line = (lax.broadcasted_iota(jnp.int32, (2 * pad, rows), 0) + parity * (2 * pad)).astype(F32)
    place = jnp.where(line == target_ref[...], 1.0, 0.0).astype(BF16)
    block = ret_ref[:, :, pl.ds(pair, 1)].astype(F32).reshape(rows, chans).astype(BF16)
    filtered = dot(table_ref[...], dot(place, block).astype(BF16))
    out_ref[0] = (normed_ref[a].astype(F32) + filtered).astype(BF16)


def per_device(field, gain, slot_wave, legendre, mixing):
    count = lax.axis_size("lat")
    lat_dev, width, chans = field.shape
    slot_dev, degs, nlat = legendre.shape
    groups, lat_pairs = slot_dev // 2, lat_dev // 2
    table, pad = wave_table(degs, width)
    tsum = table.astype(np.float64).sum(axis=1).astype(np.float32)
    rows = count * 8
    vmem = pl.BlockSpec(memory_space=pltpu.VMEM)
    hbm = pl.BlockSpec(memory_space=pltpu.HBM)
    dma = pltpu.SemaphoreType.DMA
    half_limit = 30 * 2**20
    block = (groups, count, lat_pairs, 8, chans)
    ret, target, normed = pl.pallas_call(
        functools.partial(exchange_kernel, count, pad),
        out_shape=(
            jax.ShapeDtypeStruct(block, BF16),
            jax.ShapeDtypeStruct((1, groups * rows), F32),
            jax.ShapeDtypeStruct(field.shape, BF16),
        ),
        in_specs=[hbm] * 8,
        out_specs=(vmem, vmem, vmem),
        scratch_shapes=[
            pltpu.SMEM(slot_wave.shape, jnp.int32),
            pltpu.VMEM((1,) + slot_wave.shape, jnp.int32),
            pltpu.VMEM((1, chans), F32),
            pltpu.VMEM(table.shape, BF16),
            pltpu.VMEM((1, 2 * pad), F32),
            pltpu.VMEM(legendre.shape, BF16),
            pltpu.VMEM(mixing.shape, BF16),
            pltpu.VMEM((groups, rows, 4 * pad), BF16),
            pltpu.VMEM((lat_dev, 2 * pad, chans), F32),
            pltpu.VMEM((lat_pairs, 4 * pad, chans), BF16),
            pltpu.VMEM(block, BF16),
            pltpu.VMEM(block, BF16),
            pltpu.VMEM(block, BF16),
            pltpu.VMEM((2, chans), F32),
            pltpu.VMEM((count, 2, chans), F32),
            pltpu.VMEM((groups, 4 * degs, 4 * nlat), BF16),
            dma((lat_dev,)),
            dma((7,)),
            dma((2,)),
            dma((2, groups)),
            dma((2, groups)),
        ],
        compiler_params=pltpu.CompilerParams(
            collective_id=0, has_side_effects=True, vmem_limit_bytes=half_limit if count <= 16 else 2 * half_limit
        ),
        name="exchange",
    )(*(pltpu.with_memory_space_constraint(x, pltpu.HBM) for x in (
        field, slot_wave, slot_wave.reshape(1, -1), gain.reshape(1, chans), jnp.asarray(table),
        jnp.asarray(tsum.reshape(1, -1)), legendre, mixing,
    )))
    return pl.pallas_call(
        functools.partial(inverse_kernel, pad),
        grid=(lat_dev,),
        out_shape=jax.ShapeDtypeStruct(field.shape, BF16),
        in_specs=[vmem, vmem, vmem, vmem],
        out_specs=pl.BlockSpec((1, width, chans), lambda a: (a, 0, 0)),
        compiler_params=pltpu.CompilerParams(vmem_limit_bytes=half_limit),
        name="inverse",
    )(ret, target, jnp.asarray(table.T.copy()), normed)


def solution(mesh):
    return jax.shard_map(
        per_device,
        mesh=mesh,
        in_specs=(
            P(("member", "lat"), None, None),
            P(),
            P(),
            P("lat", None, None),
            P("lat", None, None, None),
        ),
        out_specs=P(("member", "lat"), None, None),
        check_vma=False,
    )
```
